32 devices in a mesh: dp: 4 (over z), row: 2 (over y), fsdp: 4 (over x, core).
Axes of the slice: x: 2, y: 2, z: 4, core: 2. Of those that a mesh axis runs over, the one named last changes fastest.
Arguments:
- x_saved: bfloat16 [2, 49152, 288], P(None, ('dp', 'row', 'fsdp'))
- dy_out: bfloat16 [2, 49152, 288], P(None, ('dp', 'row', 'fsdp'))
- w_gate: bfloat16 [288, 768], P(None, ('row', 'fsdp'))
- w_up: bfloat16 [288, 768], P(None, ('row', 'fsdp'))
- w_down: bfloat16 [768, 288], P(('row', 'fsdp'))
- g_next: float32 [32, 3, 288, 768], P(('dp', 'row', 'fsdp'))
Outputs:
- output 1: bfloat16 [2, 49152, 288], P(None, ('dp', 'row', 'fsdp'))
- output 2: float32 [3, 288, 768], P(None, None, ('row', 'fsdp'))
- output 3: float32 [32, 3, 288, 768], P(('dp', 'row', 'fsdp'))
All inputs are finite; a program needn't handle non-finite values.
Results may differ from the reference program's by a relative error of at most 0.0105422.
Values are sent between devices in bfloat16 or wider.
A program may use at most 1 GiB of HBM per device.

```python
import jax
import jax.numpy as jnp
from jax import lax

DEVICES = 32
TOK_DEV = 1536
D_MODEL = 288
FF_DIM = 768
MICRO_COUNT = 2


def setup_inputs(seed: int = 0) -> dict:
    key_list = jax.random.split(jax.random.key(seed), 6)
    tok_all = DEVICES * TOK_DEV
    act_shape = (MICRO_COUNT, tok_all, D_MODEL)
    x_saved = jax.random.normal(key_list[0], act_shape, jnp.float32)
    dy_out = jax.random.normal(key_list[1], act_shape, jnp.float32)
    w_gate = jax.random.normal(key_list[2], (D_MODEL, FF_DIM), jnp.float32) * D_MODEL ** -0.5
    w_up = jax.random.normal(key_list[3], (D_MODEL, FF_DIM), jnp.float32) * D_MODEL ** -0.5
    w_down = jax.random.normal(key_list[4], (FF_DIM, D_MODEL), jnp.float32) * FF_DIM ** -0.5
    g_next = jax.random.normal(key_list[5], (DEVICES, 3, D_MODEL, FF_DIM), jnp.float32) * DEVICES ** -0.5
    return {"x_saved": x_saved.astype(jnp.bfloat16), "dy_out": dy_out.astype(jnp.bfloat16), "w_gate": w_gate.astype(jnp.bfloat16), "w_up": w_up.astype(jnp.bfloat16), "w_down": w_down.astype(jnp.bfloat16), "g_next": g_next}


def silu_slope(pre_act):
    sigmoid_val = jax.nn.sigmoid(pre_act)
    return sigmoid_val * (1.0 + pre_act * (1.0 - sigmoid_val))


def device_backward(x_dev, dy_dev, w_gate, w_up, w_down):
    def one_micro(grad_acc, micro_pair):
        x_mb, dy_mb = micro_pair
        pre_gate = jnp.dot(x_mb, w_gate, preferred_element_type=jnp.float32)
        pre_up = jnp.dot(x_mb, w_up, preferred_element_type=jnp.float32)
        act_gate = jax.nn.silu(pre_gate)
        hidden = (act_gate * pre_up).astype(jnp.bfloat16)
        d_hidden = jnp.dot(dy_mb, w_down.T, preferred_element_type=jnp.float32)
        d_gate = (d_hidden * pre_up * silu_slope(pre_gate)).astype(jnp.bfloat16)
        d_up = (d_hidden * act_gate).astype(jnp.bfloat16)
        dx_mb = (jnp.dot(d_gate, w_gate.T, preferred_element_type=jnp.float32) + jnp.dot(d_up, w_up.T, preferred_element_type=jnp.float32)).astype(jnp.bfloat16)
        grad_mb = jnp.stack([
            jnp.dot(x_mb.T, d_gate, preferred_element_type=jnp.float32),
            jnp.dot(x_mb.T, d_up, preferred_element_type=jnp.float32),
            jnp.dot(dy_mb.T, hidden, preferred_element_type=jnp.float32),
        ])
        return grad_acc + grad_mb, dx_mb

    grad_init = jnp.zeros((3, D_MODEL, FF_DIM), jnp.float32)
    grad_sum, dx_dev = lax.scan(one_micro, grad_init, (x_dev, dy_dev))
    return dx_dev, grad_sum


def reference(x_saved, dy_out, w_gate, w_up, w_down, g_next):
    x_dev = x_saved.reshape(MICRO_COUNT, DEVICES, TOK_DEV, D_MODEL).transpose(1, 0, 2, 3)
    dy_dev = dy_out.reshape(MICRO_COUNT, DEVICES, TOK_DEV, D_MODEL).transpose(1, 0, 2, 3)

    def per_device(dev_pair):
        return device_backward(dev_pair[0], dev_pair[1], w_gate, w_up, w_down)

    dx_dev, grad_layer = lax.map(per_device, (x_dev, dy_dev))
    dx_out = dx_dev.transpose(1, 0, 2, 3).reshape(MICRO_COUNT, DEVICES * TOK_DEV, D_MODEL)
    grad_next = jnp.sum(g_next.astype(jnp.bfloat16).astype(jnp.float32), axis=0)
    return dx_out, grad_next, grad_layer
```

```python
import functools
import jax
import jax.numpy as jnp
from jax import lax
from jax.experimental import pallas as pl
from jax.experimental.pallas import tpu as pltpu
from jax.sharding import PartitionSpec as P

TOK_AXES = ("dp", "row", "fsdp")
GROUP_AXES = ("row", "fsdp")
MESH = pl.DeviceIdType.MESH
BF = jnp.bfloat16
F32 = jnp.float32

D = 288
FF = 768
SH = 96
LW = 896
FC = 256
TT = 512
MTOK = 1536
PIECES = ((0, 256), (256, 512), (512, 896))
NT_DIMS = (((1,), (1,)), ((), ()))
CUTS = (
    (0, 0, 0, 0, 96), (0, 96, 1, 0, 96), (0, 192, 2, 0, 64),
    (1, 0, 2, 64, 32), (1, 32, 3, 0, 96), (1, 128, 4, 0, 96), (1, 224, 5, 0, 32),
    (2, 0, 5, 32, 64), (2, 64, 6, 0, 96), (2, 160, 7, 0, 96),
)


def dot(a, b):
    return jnp.dot(a, b, preferred_element_type=F32)


def dot_nt(a, b):
    return lax.dot_general(a, b, NT_DIMS, preferred_element_type=F32)


def eye(n):
    r = lax.broadcasted_iota(jnp.int32, (n, n), 0)
    c = lax.broadcasted_iota(jnp.int32, (n, n), 1)
    return (r == c).astype(F32).astype(BF)


def body(x_hbm, dy_hbm, wg_hbm, wu_hbm, wd_hbm, g_hbm,
         dx_hbm, gn_ref, dw_hbm,
         xt, yt, wg, wu, wd, g32, wire, xtail, wn, hh, dxacc, dxo, dwa,
         gt, gr, s1, r1, s2, r2, zb,
         in_sem, out_sem, ws_sem, wrd_sem, wrp_sem, gs_sem, gr_sem, zs_sem, zr_sem):
    z = lax.axis_index("dp")
    y = lax.axis_index("row")
    f = lax.axis_index("fsdp")
    x = f // 2
    c = f % 2
    partner = (z, y, f + 1 - 2 * c)
    nbr_a = (z, y + (1 - c) * (1 - 2 * y), (f + 2 * c) % 4)
    nbr_b = (z, y + c * (1 - 2 * y), (f + 2 * (1 - c)) % 4)
    ax_a = 1 - c
    ax_b = c

    loads = [
        pltpu.make_async_copy(wg_hbm, wg, in_sem.at[0]),
        pltpu.make_async_copy(wu_hbm, wu, in_sem.at[1]),
        pltpu.make_async_copy(wd_hbm, wd, in_sem.at[2]),
        pltpu.make_async_copy(g_hbm.at[0, 0], g32.at[0], in_sem.at[3]),
        pltpu.make_async_copy(g_hbm.at[0, 1], g32.at[1], in_sem.at[4]),
        pltpu.make_async_copy(g_hbm.at[0, 2], g32.at[2], in_sem.at[5]),
        pltpu.make_async_copy(x_hbm, xt, in_sem.at[6]),
        pltpu.make_async_copy(dy_hbm, yt, in_sem.at[7]),
    ]
    for l in loads:
        l.start()

    bar = pltpu.get_barrier_semaphore()
    for dev in (partner, nbr_a, nbr_b):
        pl.semaphore_signal(bar, inc=1, device_id=dev, device_id_type=MESH)

    @pl.when(z > 0)
    def _():
        pl.semaphore_signal(bar, inc=1, device_id=(z - 1, y, f), device_id_type=MESH)

    @pl.when(z < 3)
    def _():
        pl.semaphore_signal(bar, inc=1, device_id=(z + 1, y, f), device_id_type=MESH)

    def rows_of(yy, xx, cc):
        return pl.ds(pl.multiple_of((4 * yy + 2 * xx + cc) * SH, 32), SH)

    own = rows_of(y, x, c)
    i96 = eye(SH)
    for l in loads[:3]:
        l.wait()
    wire[own, 0:256] = dot_nt(i96, wg[0:256, :]).astype(BF)
    wire[own, 256:512] = dot_nt(i96, wu[0:256, :]).astype(BF)
    wire[own, 512:768] = wd[:, 0:256]
    tails = dot_nt(i96, jnp.concatenate([wg[256:288, :], wu[256:288, :]], 0)).astype(BF)
    wire[own, 768:896] = jnp.concatenate([tails, wd[:, 256:288], jnp.zeros((SH, 32), BF)], 1)

    @pl.when(jnp.logical_and(z > 0, z < 3))
    def _():
        pl.semaphore_wait(bar, 5)

    @pl.when(jnp.logical_or(z == 0, z == 3))
    def _():
        pl.semaphore_wait(bar, 4)

    def wcopy(rows, send, recv, dev):
        return pltpu.make_async_remote_copy(
            src_ref=wire.at[rows], dst_ref=wire.at[rows], send_sem=ws_sem.at[send], recv_sem=recv,
            device_id=dev, device_id_type=MESH)

    rows_x = rows_of(y, 1 - x, c)
    rows_y = rows_of(1 - y, x, c)
    rows_d = rows_of(1 - y, 1 - x, c)
    ya = y + ax_a * (1 - 2 * y)
    xa = x + ax_b * (1 - 2 * x)
    yb = y + ax_b * (1 - 2 * y)
    xb = x + ax_a * (1 - 2 * x)
    rows_a = rows_of(ya, xa, c)
    rows_b = rows_of(yb, xb, c)
    w_own_a = wcopy(own, 0, wrd_sem.at[ax_a], nbr_a)
    w_own_b = wcopy(own, 1, wrd_sem.at[ax_b], nbr_b)
    w_own_p = wcopy(own, 2, wrp_sem.at[0], partner)
    w_fa_p = wcopy(rows_a, 3, wrp_sem.at[1 + ax_a], partner)
    w_fa_b = wcopy(rows_a, 4, wrd_sem.at[2], nbr_b)
    w_fb_p = wcopy(rows_b, 5, wrp_sem.at[1 + ax_b], partner)
    w_fd_p = wcopy(rows_d, 6, wrp_sem.at[3], partner)

    def wrecv(rows, sem):
        wcopy(rows, 0, sem, partner).wait_recv()

    w_own_a.start()
    w_own_b.start()
    w_own_p.start()

    i256 = eye(256)
    for s in range(3):
        loads[3 + s].wait()
        for fb in range(3):
            t = dot_nt(i256, g32[s, 0:256, 256 * fb:256 * fb + 256].astype(BF)).astype(BF)
            for blk, r0, sh, r, n in CUTS:
                if blk == fb:
                    gt[sh // 2, sh % 2, r:r + n, 256 * s:256 * s + 256] = t[r0:r0 + n]
        if s == 2:
            for fb in range(3):
                tl = jnp.concatenate([g32[k, 256:288, 256 * fb:256 * fb + 256].astype(BF) for k in range(3)]
                                     + [jnp.zeros((32, 256), BF)], 0)
                t = dot_nt(i256, tl).astype(BF)
                for blk, r0, sh, r, n in CUTS:
                    if blk == fb:
                        gt[sh // 2, sh % 2, r:r + n, 768:896] = t[r0:r0 + n]
        g_pair(gt, gr, gs_sem, gr_sem, s, c, partner).start()

    loads[6].wait()
    loads[7].wait()
    for m in range(2):
        sl = slice(m * MTOK, (m + 1) * MTOK)
        xtl = xt[m, 256:288]
        xtail[0, :, sl] = jnp.concatenate([xtl, jnp.zeros((96, MTOK), BF)], 0)
        xtail[1, :, sl] = jnp.concatenate([jnp.zeros((32, MTOK), BF), xtl, jnp.zeros((64, MTOK), BF)], 0)
        xtail[2, :, sl] = jnp.concatenate([jnp.zeros((64, MTOK), BF), yt[m, 256:288], jnp.zeros((32, MTOK), BF)], 0)

    def chip(ra, rb):
        ya_ = y + (1 - 2 * y) * (ra * ax_a + rb * ax_b)
        xa_ = x + (1 - 2 * x) * (ra * ax_b + rb * ax_a)
        return 2 * ya_ + xa_

    def add(p, q):
        return (p.astype(F32) + q.astype(F32)).astype(BF)

    def remote(src, dst, ssem, rsem, dev):
        return pltpu.make_async_remote_copy(src_ref=src, dst_ref=dst, send_sem=ssem, recv_sem=rsem,
                                            device_id=dev, device_id_type=MESH)

    def ph1(p):
        lo, hi = PIECES[p]
        return remote(s1.at[1, :, :, lo:hi], r1.at[:, :, lo:hi], gs_sem.at[3 + p], gr_sem.at[3 + p], nbr_a)

    def ph2(p):
        lo, hi = PIECES[p]
        return remote(s2.at[1, :, lo:hi], r2.at[:, lo:hi], gs_sem.at[6 + p], gr_sem.at[6 + p], nbr_b)

    def zcopy(slot, p, send, dz):
        lo, hi = PIECES[p]
        return remote(zb.at[slot, :, lo:hi], zb.at[slot, :, lo:hi], zs_sem.at[send, p], zr_sem.at[slot, p], (z + dz, y, f))

    def ev_pair(p):
        lo, hi = PIECES[p]
        g_pair(gt, gr, gs_sem, gr_sem, p, c, partner).wait_recv()
        for ra in (1, 0):
            for rb in range(2):
                q = chip(ra, rb)
                s1[ra, rb, :, lo:hi] = add(gt[q, c, :, lo:hi], gr[q, :, lo:hi])
        ph1(p).start()

    def ev_ph1(p):
        lo, hi = PIECES[p]
        ph1(p).wait_recv()
        for rb in (1, 0):
            s2[rb, :, lo:hi] = add(s1[0, rb, :, lo:hi], r1[rb, :, lo:hi])
        ph2(p).start()

    def ev_ph2(p):
        lo, hi = PIECES[p]
        ph2(p).wait_recv()
        zb[z, :, lo:hi] = add(s2[0, :, lo:hi], r2[:, lo:hi])

        @pl.when(z < 3)
        def _():
            zcopy(z, p, 0, 1).start()

        @pl.when(z > 0)
        def _():
            zcopy(z, p, 1, -1).start()

    def ev_z(h, p):
        @pl.when(z >= h)
        def _():
            zcopy(z - h, p, 0, 0 if False else 1).wait_recv()
            if h < 3:
                @pl.when(z < 3)
                def _():
                    zcopy(z - h, p, 2 * h, 1).start()

        @pl.when(z + h <= 3)
        def _():
            zcopy(z + h, p, 0, 1).wait_recv()
            if h < 3:
                @pl.when(z > 0)
                def _():
                    zcopy(z + h, p, 2 * h + 1, -1).start()

    def ev_final():
        t = zb[0].astype(F32) + zb[1].astype(F32) + zb[2].astype(F32) + zb[3].astype(F32)
        t = jnp.concatenate([t, jnp.zeros((32, LW), F32)], 0).T
        for s in range(3):
            gn_ref[s, 0:256, :] = t[256 * s:256 * s + 256, 0:SH]
            gn_ref[s, 256:288, :] = t[768 + 32 * s:800 + 32 * s, 0:SH]

    for p in range(3):
        ev_pair(p)
    wrecv(rows_b, wrd_sem.at[ax_b])
    w_fb_p.start()
    wrecv(rows_a, wrd_sem.at[ax_a])
    w_fa_b.start()
    w_fa_p.start()
    wrecv(rows_of(y, x, 1 - c), wrp_sem.at[0])
    wrecv(rows_of(y, 1 - x, 1 - c), wrp_sem.at[1])

    def ev_diag():
        wrecv(rows_d, wrd_sem.at[2])
        w_fd_p.start()

    def ev_rest():
        wrecv(rows_of(1 - y, x, 1 - c), wrp_sem.at[2])
        wrecv(rows_of(1 - y, 1 - x, 1 - c), wrp_sem.at[3])

    nt = 2 * MTOK // TT
    per = MTOK // TT

    events = {}

    def at(step, fn, *args):
        events.setdefault(step, []).append((fn, args))

    at(2, ev_diag)
    for p in range(3):
        at(1 + p, ev_ph1, p)
        at(3 + p, ev_ph2, p)
        at(6 + p, ev_z, 1, p)
        at(9 + p, ev_z, 2, p)
        at(12 + p, ev_z, 3, p)
    at(15, ev_final)
    at(nt, ev_rest)

    def step(it, carry):
        for k, evs in sorted(events.items()):
            @pl.when(it == k)
            def _():
                for fn, args in evs:
                    fn(*args)
        j = it // nt
        i = it % nt
        ch = j + y * (2 - 2 * j)
        rows = pl.ds(pl.multiple_of(ch * FC, FC), FC)

        @pl.when(i == 0)
        def _():
            e = eye(FC)
            t = dot_nt(e[:128, :128], wire[rows, 768:896]).astype(BF)
            for k in range(2):
                wn[k, 0:256, :] = dot_nt(e, wire[rows, 256 * k:256 * k + 256]).astype(BF)
                wn[k, 256:288, :] = t[32 * k:32 * k + 32]

        m = i // per
        col = pl.ds(pl.multiple_of((i % per) * TT, TT), TT)
        gcol = pl.ds(pl.multiple_of(i * TT, TT), TT)
        tl = wire[rows, 768:896]
        a = dot(wire[rows, 0:256], xt[m, 0:256, col]) + dot(tl, xtail[0, :, gcol])
        b = dot(wire[rows, 256:512], xt[m, 0:256, col]) + dot(tl, xtail[1, :, gcol])
        dh = dot(wire[rows, 512:768], yt[m, 0:256, col]) + dot(tl, xtail[2, :, gcol])
        s = 1.0 / (1.0 + jnp.exp(-a))
        act = a * s
        hh[0] = (dh * b * (s + act * (1.0 - s))).astype(BF)
        hh[1] = (dh * act).astype(BF)
        hh[2] = (act * b).astype(BF)
        d = dot(wn[0], hh[0]) + dot(wn[1], hh[1])

        @pl.when(j == 0)
        def _():
            dxacc[m, :, col] = d

        @pl.when(j == 1)
        def _():
            dxacc[m, :, col] = d + dxacc[m, :, col]

        @pl.when(j == 2)
        def _():
            dxo[m, :, col] = (d + dxacc[m, :, col]).astype(BF)
        for k in range(3):
            o = dot_nt(xt[m, :, col] if k < 2 else yt[m, :, col], hh[k])
            dwa[k, :, rows] = jnp.where(i == 0, o, o + dwa[k, :, rows])

        @pl.when(i == nt - 1)
        def _():
            out_dw(j, rows).start()

        @pl.when(jnp.logical_and(j == 2, i % per == per - 1))
        def _():
            pltpu.make_async_copy(dxo.at[m], dx_hbm.at[m], out_sem.at[3 + m]).start()
        return carry

    def out_dw(j, rows):
        return pltpu.make_async_copy(dwa.at[:, :, rows], dw_hbm.at[0, :, :, rows], out_sem.at[j])

    lax.fori_loop(0, 3 * nt, step, 0)

    for j in range(3):
        ch = j + y * (2 - 2 * j)
        out_dw(j, pl.ds(pl.multiple_of(ch * FC, FC), FC)).wait()
    for m in range(2):
        pltpu.make_async_copy(dxo.at[m], dx_hbm.at[m], out_sem.at[3 + m]).wait()
    for cp in (w_own_a, w_own_b, w_own_p, w_fa_p, w_fa_b, w_fb_p, w_fd_p):
        cp.wait_send()
    for p in range(3):
        g_pair(gt, gr, gs_sem, gr_sem, p, c, partner).wait_send()
        ph1(p).wait_send()
        ph2(p).wait_send()

        @pl.when(z < 3)
        def _():
            zcopy(z, p, 0, 1).wait_send()

        @pl.when(z > 0)
        def _():
            zcopy(z, p, 1, -1).wait_send()
        for h in (1, 2):
            @pl.when(jnp.logical_and(z >= h, z < 3))
            def _():
                zcopy(z - h, p, 2 * h, 1).wait_send()

            @pl.when(jnp.logical_and(z + h <= 3, z > 0))
            def _():
                zcopy(z + h, p, 2 * h + 1, -1).wait_send()


def g_pair(gt, gr, gs_sem, gr_sem, p, c, partner):
    lo, hi = PIECES[p]
    return pltpu.make_async_remote_copy(
        src_ref=gt.at[:, 1 - c, :, lo:hi], dst_ref=gr.at[:, :, lo:hi], send_sem=gs_sem.at[p], recv_sem=gr_sem.at[p],
        device_id=partner, device_id_type=MESH)


def fused(x_t, dy_t, wg, wu, wd, g):
    any_ = pl.BlockSpec(memory_space=pl.ANY)
    vm = pl.BlockSpec(memory_space=pltpu.VMEM)
    dma = pltpu.SemaphoreType.DMA
    return pl.pallas_call(
        body,
        name="mlp_bwd",
        out_shape=[
            jax.ShapeDtypeStruct((2, D, MTOK), BF),
            jax.ShapeDtypeStruct((3, D, SH), F32),
            jax.ShapeDtypeStruct((1, 3, D, FF), F32),
        ],
        in_specs=[any_] * 6,
        out_specs=[any_, vm, any_],
        scratch_shapes=[
            pltpu.VMEM((2, D, MTOK), BF), pltpu.VMEM((2, D, MTOK), BF),
            pltpu.VMEM((D, SH), BF), pltpu.VMEM((D, SH), BF), pltpu.VMEM((SH, D), BF),
            pltpu.VMEM((3, D, FF), F32),
            pltpu.VMEM((FF, LW), BF),
            pltpu.VMEM((3, 128, 2 * MTOK), BF),
            pltpu.VMEM((2, D, FC), BF),
            pltpu.VMEM((3, FC, TT), BF),
            pltpu.VMEM((2, D, MTOK), F32),
            pltpu.VMEM((2, D, MTOK), BF),
            pltpu.VMEM((3, D, FF), F32),
            pltpu.VMEM((4, 2, SH, LW), BF),
            pltpu.VMEM((4, SH, LW), BF),
            pltpu.VMEM((2, 2, SH, LW), BF),
            pltpu.VMEM((2, SH, LW), BF),
            pltpu.VMEM((2, SH, LW), BF),
            pltpu.VMEM((SH, LW), BF),
            pltpu.VMEM((4, SH, LW), BF),
            dma((8,)), dma((5,)), dma((7,)), dma((3,)), dma((4,)), dma((9,)), dma((9,)), dma((6, 3)), dma((4, 3)),
        ],
        compiler_params=pltpu.CompilerParams(
            collective_id=0, has_side_effects=True, vmem_limit_bytes=60 * 1024 * 1024),
        cost_estimate=pl.CostEstimate(flops=11_000_000_000, bytes_accessed=12_000_000, transcendentals=5_000_000),
    )(x_t, dy_t, wg, wu, wd, g)


def solution(mesh):
    def local_step(x_dev, dy_dev, gate_shard, up_shard, down_shard, g_dev):
        dx_t, grad_next, grad_layer = fused(
            jnp.swapaxes(x_dev, 1, 2), jnp.swapaxes(dy_dev, 1, 2), gate_shard, up_shard, down_shard, g_dev)
        return jnp.swapaxes(dx_t, 1, 2), grad_next, grad_layer

    in_specs = (P(None, TOK_AXES, None), P(None, TOK_AXES, None), P(None, GROUP_AXES), P(None, GROUP_AXES), P(GROUP_AXES, None), P(TOK_AXES, None, None, None))
    out_specs = (P(None, TOK_AXES, None), P(None, None, GROUP_AXES), P(TOK_AXES, None, None, None))
    return jax.shard_map(local_step, mesh=mesh, in_specs=in_specs, out_specs=out_specs, check_vma=False)
```

```python
import functools
import jax
import jax.numpy as jnp
from jax import lax
from jax.experimental import pallas as pl
from jax.experimental.pallas import tpu as pltpu
from jax.sharding import PartitionSpec as P

TOK_AXES = ("dp", "row", "fsdp")
GROUP_AXES = ("row", "fsdp")
MESH = pl.DeviceIdType.MESH
BF = jnp.bfloat16
F32 = jnp.float32

D = 288
FF = 768
SH = 96
LW = 896
FC = 256
TT = 256
MTOK = 1536
PIECES = ((0, 2), (2, 4), (4, 7))
NP = len(PIECES)
SUMMED = (0, 1)
NL = LW // 128
NT_DIMS = (((1,), (1,)), ((), ()))
CUTS = (
    (0, 0, 0, 0, 96), (0, 96, 1, 0, 96), (0, 192, 2, 0, 64),
    (1, 0, 2, 64, 32), (1, 32, 3, 0, 96), (1, 128, 4, 0, 96), (1, 224, 5, 0, 32),
    (2, 0, 5, 32, 64), (2, 64, 6, 0, 96), (2, 160, 7, 0, 96),
)


def dot(a, b):
    return jnp.dot(a, b, preferred_element_type=F32)


def dot_nt(a, b):
    return lax.dot_general(a, b, NT_DIMS, preferred_element_type=F32)


def eye(n):
    r = lax.broadcasted_iota(jnp.int32, (n, n), 0)
    c = lax.broadcasted_iota(jnp.int32, (n, n), 1)
    return (r == c).astype(F32).astype(BF)


PRE = ("send_p", "send_64", "send_y.0", "send_y.1", "g.0", "g.1", "g.2", "send_x.0", "send_x.1", "tails", "own_p",)
EVENTS = {
    2: ("pair.0", "pair.1", "pair.2",),
    8: ("pass64",),
    11: ("x64",),
    23: ("ph1.0", "ph1.1", "y",),
    27: ("ph1.2", "xrest",),
    30: ("ph2.0", "ph2.1", "rest2",),
    36: ("ph2.2",),
    42: ("diag", "relay.0",),
    49: ("rest3", "relay.1",),
    55: ("relay.2",),
    68: ("zall.0", "zall.1", "zall.2",),
}


def body(x_hbm, dy_hbm, wg_hbm, wu_hbm, wd_hbm, g_hbm,
         dx_ref, dw_ref, zb, tot,
         xt, yt, hh, wn, dxacc, wg, wu, wd, g32, wire, wc, xtail,
         gt, gr, s1, r1, s2, r2,
         in_sem, ws_sem, wrd_sem, wrp_sem, gs_sem, gr_sem, zs_sem, zr_sem, ts_sem, tr_sem):
    z = lax.axis_index("dp")
    y = lax.axis_index("row")
    f = lax.axis_index("fsdp")
    x = f // 2
    c = f % 2
    ny = 1 - y
    partner = (z, y, f + 1 - 2 * c)
    nbr_x = (z, y, (f + 2) % 4)
    nbr_y = (z, ny, f)
    nbr_a = (z, y + (1 - c) * (1 - 2 * y), (f + 2 * c) % 4)
    nbr_b = (z, y + c * (1 - 2 * y), (f + 2 * (1 - c)) % 4)
    ax_a = 1 - c
    ax_b = c
    split = c == 1 - x
    gets = c == x

    g_loads = [pltpu.make_async_copy(g_hbm.at[0, k], g32.at[k], in_sem.at[k]) for k in range(3)]
    w_loads = [
        pltpu.make_async_copy(wg_hbm, wg, in_sem.at[9]),
        pltpu.make_async_copy(wu_hbm, wu, in_sem.at[10]),
        pltpu.make_async_copy(wd_hbm, wd, in_sem.at[11]),
    ]
    x_loads = [
        pltpu.make_async_copy(x_hbm, xt, in_sem.at[12]),
        pltpu.make_async_copy(dy_hbm, yt, in_sem.at[13]),
    ]
    for l in w_loads + g_loads + x_loads:
        l.start()

    bar = pltpu.get_barrier_semaphore()
    for dev in (partner, nbr_a, nbr_b):
        pl.semaphore_signal(bar, inc=1, device_id=dev, device_id_type=MESH)

    mid = jnp.logical_or(z == 1, z == 2)
    end = jnp.logical_not(mid)
    near = jnp.where(z == 0, 1, jnp.where(z == 3, 2, 3 - z))
    far = jnp.where(z == 0, 2, jnp.where(z == 3, 1, jnp.where(z == 1, 3, 0)))
    mine = jnp.where(z == 1, 0, 3)

    pl.semaphore_signal(bar, inc=1, device_id=(near, y, f), device_id_type=MESH)
    pl.semaphore_signal(bar, inc=1, device_id=(far, y, f), device_id_type=MESH)

    @pl.when(mid)
    def _():
        pl.semaphore_signal(bar, inc=1, device_id=(mine, y, f), device_id_type=MESH)

    def ds(start, n):
        return pl.ds(pl.multiple_of(start, 32), n)

    def rows_of(yy, xx, cc):
        return ds((4 * yy + 2 * xx + cc) * SH, SH)

    own = rows_of(y, x, c)
    i96 = eye(SH)
    for l in w_loads:
        l.wait()
    wire[own, 0:256] = dot_nt(i96, wg[0:256, :]).astype(BF)
    wire[own, 256:512] = dot_nt(i96, wu[0:256, :]).astype(BF)
    wire[own, 512:768] = wd[:, 0:256]
    tails = dot_nt(i96, jnp.concatenate([wg[256:288, :], wu[256:288, :]], 0)).astype(BF)
    wire[own, 768:896] = jnp.concatenate([tails, wd[:, 256:288], jnp.zeros((SH, 32), BF)], 1)

    @pl.when(mid)
    def _():
        pl.semaphore_wait(bar, 6)

    @pl.when(end)
    def _():
        pl.semaphore_wait(bar, 5)

    def remote(src, dst, ssem, rsem, dev):
        return pltpu.make_async_remote_copy(src_ref=src, dst_ref=dst, send_sem=ssem, recv_sem=rsem,
                                            device_id=dev, device_id_type=MESH)

    def wcopy(rows, send, recv, dev):
        return remote(wire.at[rows], wire.at[rows], ws_sem.at[send], recv, dev)

    def wrecv(rows, sem):
        wcopy(rows, 0, sem, partner).wait_recv()

    def r64(xs):
        return ds(384 * y + 128 + 64 * xs, 64)

    def r32(xs):
        return ds(384 * y + 96 + 160 * xs, 32)

    sends = []

    def start(cp, cond=None):
        sends.append((cp, cond))
        if cond is None:
            cp.start()
        else:
            @pl.when(cond)
            def _():
                cp.start()

    def ev_send_p():
        start(wcopy(own, 1, wrp_sem.at[0], partner))

    def ev_send_64():
        start(wcopy(r64(x), 0, wrd_sem.at[0], nbr_x), split)

    def ev_send_y(core):
        start(wcopy(own, 2, wrd_sem.at[2], nbr_y), c == core)

    def ev_send_x(part):
        if part == 0:
            start(wcopy(r32(x), 3, wrd_sem.at[1], nbr_x), split)
        else:
            start(wcopy(own, 3, wrd_sem.at[1], nbr_x), jnp.logical_not(split))

    i256 = eye(256)

    def pair_copy(p):
        lo, hi = PIECES[p]
        return remote(gt.at[lo:hi, :, 1 - c], gr.at[lo:hi], gs_sem.at[p], gr_sem.at[p], partner)

    def put(o, fb, t):
        for blk, r0, sh, r, m in CUTS:
            if blk == fb:
                gt[t, sh // 2, sh % 2, r:r + m, :] = o[r0:r0 + m]

    def ready(*tiles):
        for p in range(NP):
            if PIECES[p][1] - 1 in tiles:
                start(pair_copy(p))

    def ev_g(k):
        g_loads[k].wait()
        for fb in range(3):
            o = dot_nt(i256, g32[k, 0:256, 256 * fb:256 * fb + 256].astype(BF)).astype(BF)
            put(o[:, 0:128], fb, 2 * k)
            put(o[:, 128:256], fb, 2 * k + 1)
        if k == 2:
            for fb in range(3):
                tl = jnp.concatenate([g32[j, 256:288, 256 * fb:256 * fb + 256].astype(BF) for j in range(3)]
                                     + [jnp.zeros((32, 256), BF)], 0)
                put(dot_nt(i256, tl).astype(BF), fb, 6)
        ready(*((2 * k, 2 * k + 1) if k < 2 else (4, 5, 6)))

    def ev_tails():
        for l in x_loads:
            l.wait()
        for m in range(2):
            xtl = xt[m, 256:288]
            xtail[0, m] = jnp.concatenate([xtl, jnp.zeros((96, MTOK), BF)], 0)
            xtail[1, m] = jnp.concatenate([jnp.zeros((32, MTOK), BF), xtl, jnp.zeros((64, MTOK), BF)], 0)
            xtail[2, m] = jnp.concatenate([jnp.zeros((64, MTOK), BF), yt[m, 256:288], jnp.zeros((32, MTOK), BF)], 0)

    def chip(ra, rb):
        ya_ = y + (1 - 2 * y) * (ra * ax_a + rb * ax_b)
        xa_ = x + (1 - 2 * x) * (ra * ax_b + rb * ax_a)
        return 2 * ya_ + xa_

    def add(p, q):
        return (p.astype(F32) + q.astype(F32)).astype(BF)

    def ph1(p):
        lo, hi = PIECES[p]
        return remote(s1.at[1, lo:hi], r1.at[lo:hi], gs_sem.at[NP + p], gr_sem.at[NP + p], nbr_a)

    def ph2(p):
        lo, hi = PIECES[p]
        return remote(s2.at[1, lo:hi], r2.at[lo:hi], gs_sem.at[2 * NP + p], gr_sem.at[2 * NP + p], nbr_b)

    def zcopy(slot, p, send, dev):
        lo, hi = PIECES[p]
        return remote(zb.at[slot, lo:hi], zb.at[slot, lo:hi], zs_sem.at[send, p], zr_sem.at[slot, p], (dev, y, f))

    def ev_pair(p):
        lo, hi = PIECES[p]
        pair_copy(p).wait_recv()
        for ra in (1, 0):
            for rb in range(2):
                q = chip(ra, rb)
                s1[ra, lo:hi, rb] = add(gt[lo:hi, q, c], gr[lo:hi, q])
            if ra == 1:
                start(ph1(p))

    def ev_ph1(p):
        lo, hi = PIECES[p]
        ph1(p).wait_recv()
        s2[1, lo:hi] = add(s1[0, lo:hi, 1], r1[lo:hi, 1])
        start(ph2(p))
        s2[0, lo:hi] = add(s1[0, lo:hi, 0], r1[lo:hi, 0])

    def ev_ph2(p):
        lo, hi = PIECES[p]
        ph2(p).wait_recv()
        zb[z, lo:hi] = add(s2[0, lo:hi], r2[lo:hi])
        if p in SUMMED:
            start(zcopy(z, p, 1, far), end)
            start(zcopy(z, p, 0, near))
        else:
            start(zcopy(z, p, 1, far))
            start(zcopy(z, p, 0, near))
            start(zcopy(z, p, 2, mine), mid)

    def tcopy(p):
        lo, hi = PIECES[p]
        return remote(tot.at[lo:hi], tot.at[lo:hi], ts_sem.at[p], tr_sem.at[p], (mine, y, f))

    def ev_relay(p):
        @pl.when(mid)
        def _():
            zcopy(far, p, 0, near).wait_recv()
        if p in SUMMED:
            lo, hi = PIECES[p]

            @pl.when(mid)
            def _():
                zcopy(near, p, 0, near).wait_recv()
                zcopy(mine, p, 0, near).wait_recv()
                tot[lo:hi] = z_sum(zb, lo, hi)
            start(tcopy(p), mid)
        else:
            start(zcopy(far, p, 3, mine), mid)

    def ev_zall(p):
        if p in SUMMED:
            @pl.when(end)
            def _():
                tcopy(p).wait_recv()
        else:
            zcopy(near, p, 0, near).wait_recv()

            @pl.when(mid)
            def _():
                zcopy(mine, p, 0, near).wait_recv()

            @pl.when(end)
            def _():
                zcopy(far, p, 0, near).wait_recv()
                zcopy(3 - z, p, 0, near).wait_recv()

    def ev_own_p():
        wrecv(rows_of(y, x, 1 - c), wrp_sem.at[0])

    def ev_pass64():
        @pl.when(gets)
        def _():
            wrecv(r64(1 - x), wrd_sem.at[0])
        start(wcopy(r64(1 - x), 4, wrp_sem.at[1], partner), gets)

    def ev_x64():
        @pl.when(jnp.logical_not(gets))
        def _():
            wrecv(r64(1 - x), wrp_sem.at[1])

    def ev_xrest():
        @pl.when(gets)
        def _():
            wrecv(r32(1 - x), wrd_sem.at[1])

        @pl.when(jnp.logical_not(gets))
        def _():
            wrecv(rows_of(y, 1 - x, c), wrd_sem.at[1])
        start(wcopy(r32(1 - x), 5, wrp_sem.at[2], partner), gets)
        start(wcopy(rows_of(y, 1 - x, c), 5, wrp_sem.at[2], partner), jnp.logical_not(gets))
        start(wcopy(rows_of(y, 1 - x, c), 6, wrd_sem.at[3], nbr_y), c == 1)

    def ev_y():
        wrecv(rows_of(ny, x, c), wrd_sem.at[2])
        start(wcopy(rows_of(ny, x, c), 7, wrp_sem.at[3], partner))
        start(wcopy(rows_of(ny, x, c), 6, wrd_sem.at[3], nbr_x), c == 0)

    def ev_diag():
        wrecv(rows_of(ny, 1 - x, c), wrd_sem.at[3])
        start(wcopy(rows_of(ny, 1 - x, c), 8, wrp_sem.at[4], partner))

    def ev_rest2():
        @pl.when(gets)
        def _():
            wrecv(rows_of(y, 1 - x, 1 - c), wrp_sem.at[2])

        @pl.when(jnp.logical_not(gets))
        def _():
            wrecv(r32(1 - x), wrp_sem.at[2])
        wrecv(rows_of(ny, x, 1 - c), wrp_sem.at[3])

    def ev_rest3():
        wrecv(rows_of(ny, 1 - x, 1 - c), wrp_sem.at[4])

    handlers = {
        "pair": ev_pair, "ph1": ev_ph1, "ph2": ev_ph2, "relay": ev_relay, "zall": ev_zall, "g": ev_g, "tails": ev_tails, "send_p": ev_send_p, "send_64": ev_send_64, "send_y": ev_send_y, "send_x": ev_send_x, "own_p": ev_own_p, "x64": ev_x64, "pass64": ev_pass64,
        "xrest": ev_xrest, "y": ev_y, "diag": ev_diag, "rest2": ev_rest2, "rest3": ev_rest3,
    }

    ticks = [0]

    def run(evs):
        for ev in evs:
            name, _, arg = ev.partition(".")
            with jax.named_scope(ev.replace(".", "_")):
                handlers[name](*([int(arg)] if arg else []))

    def tick():
        run(EVENTS.get(ticks[0], ()))
        ticks[0] += 1

    def forward(w, rows, h0, n):
        for m in range(2):
            for t in range(MTOK // TT):
                forward_step(w, rows, h0, n, m, slice(t * TT, t * TT + TT))
                tick()

    def forward_step(w, rows, h0, n, m, col):
        tl = w[rows, 768:896]
        xm = xt[m, 0:256, col]
        a = dot(w[rows, 0:256], xm) + dot(tl, xtail[0, m, :, col])
        b = dot(w[rows, 256:512], xm) + dot(tl, xtail[1, m, :, col])
        dh = dot(w[rows, 512:768], yt[m, 0:256, col]) + dot(tl, xtail[2, m, :, col])
        s = 1.0 / (1.0 + jnp.exp(-a))
        act = a * s
        hh[m, ds(h0, n), col] = (dh * b * (s + act * (1.0 - s))).astype(BF)
        hh[m, ds(FC + h0, n), col] = (dh * act).astype(BF)
        hh[m, ds(2 * FC + h0, n), col] = (act * b).astype(BF)

    def natural(w, rows):
        t = dot_nt(i256[:128, :128], w[rows, 768:896]).astype(BF)
        for k in range(2):
            wn[0:256, k * FC:k * FC + FC] = dot_nt(i256, w[rows, 256 * k:256 * k + 256]).astype(BF)
            wn[256:288, k * FC:k * FC + FC] = t[32 * k:32 * k + 32]

    def backward(j, lanes):
        for m in range(2):
            for n in range(2):
                col = slice(768 * n, 768 * n + 768)
                d = dot(wn[...], hh[m, 0:2 * FC, col])
                if j == 1:
                    dxacc[m, :, col] = d
                elif j == 2:
                    dxacc[m, :, col] = d + dxacc[m, :, col]
                else:
                    dx_ref[m, :, col] = (d + dxacc[m, :, col]).astype(BF)
                tick()
        for k in range(3):
            o = grad_w(k, xt, yt, hh)
            for i, l in enumerate(lanes):
                dw_ref[0, k, :, lane_tile(l)] = o[:, 128 * i:128 * i + 128]
            tick()

    run(PRE)
    forward(wire, ds(384 * y + 192 * x, 192), 64 * x, 192)
    forward(wire, r64(1 - x), 192 * (1 - x), 64)
    first = 384 * y + 128 * x
    natural(wire, ds(first, FC))
    backward(1, (first, first + 128))

    second = (384 * y + 256 - 256 * x, 384 * ny + 256 * x)
    for i, l in enumerate(second):
        wc[128 * i:128 * i + 128] = wire[ds(l, 128)]
    full = slice(0, FC)
    forward(wc, full, 0, FC)
    natural(wc, full)
    backward(2, second)

    third = 384 * ny + 128 * (1 - x)
    forward(wire, ds(third, FC), 0, FC)
    natural(wire, ds(third, FC))
    backward(3, (third, third + 128))
    assert max(EVENTS) < ticks[0]

    for cp, cond in sends:
        if cond is None:
            cp.wait_send()
        else:
            @pl.when(cond)
            def _():
                cp.wait_send()


def lane_tile(l):
    return pl.ds(pl.multiple_of(l, 128), 128)


def grad_w(k, xt, yt, hh):
    t = yt if k == 2 else xt
    hk = slice(k * FC, k * FC + FC)
    return dot_nt(t[0], hh[0, hk]) + dot_nt(t[1], hh[1, hk])


def z_sum(zb, lo, hi):
    t = zb[0, lo:hi].astype(F32) + zb[1, lo:hi].astype(F32)
    t = t + zb[2, lo:hi].astype(F32)
    return t + zb[3, lo:hi].astype(F32)


def finish(dx, dw, zb, tot, dx_hbm, gn_hbm, dw_hbm, gno, sem):
    copies = [pltpu.make_async_copy(dw.at[0, k], dw_hbm.at[0, k], sem.at[k]) for k in range(3)]
    copies += [pltpu.make_async_copy(dx.at[m], dx_hbm.at[m], sem.at[3 + m]) for m in range(2)]
    for cp in copies:
        cp.start()
    for i in range(NL):
        piece = [lo <= i < hi for lo, hi in PIECES].index(True)
        t = tot[i] if piece in SUMMED else z_sum(zb, i, i + 1)[0]
        t = jnp.concatenate([t, jnp.zeros((32, 128), F32)], 0).T[:, 0:SH]
        if i < 6:
            gno[i // 2, 128 * (i % 2):128 * (i % 2) + 128, :] = t
        else:
            for s in range(3):
                gno[s, 256:288, :] = t[32 * s:32 * s + 32]
    copies.append(pltpu.make_async_copy(gno, gn_hbm, sem.at[5]))
    copies[-1].start()
    for cp in copies:
        cp.wait()


def fused(x_t, dy_t, wg, wu, wd, g):
    hbm = pl.BlockSpec(memory_space=pltpu.HBM)
    vm = pl.BlockSpec(memory_space=pltpu.VMEM)
    dma = pltpu.SemaphoreType.DMA
    state = [pltpu.VMEM((2, D, MTOK), BF), pltpu.VMEM((1, 3, D, FF), F32), pltpu.VMEM((4, NL, SH, 128), BF), pltpu.VMEM((NL, SH, 128), F32)]
    args = [pltpu.with_memory_space_constraint(t, pltpu.HBM) for t in (x_t, dy_t, wg, wu, wd, g)]
    mid = pl.pallas_call(
        body,
        name="mlp_bwd",
        out_shape=state,
        in_specs=[hbm] * 6,
        out_specs=[vm] * 4,
        scratch_shapes=[
            pltpu.VMEM((2, D, MTOK), BF), pltpu.VMEM((2, D, MTOK), BF),
            pltpu.VMEM((2, 3 * FC, MTOK), BF),
            pltpu.VMEM((D, 2 * FC), BF),
            pltpu.VMEM((2, D, MTOK), F32),
            pltpu.VMEM((D, SH), BF), pltpu.VMEM((D, SH), BF), pltpu.VMEM((SH, D), BF),
            pltpu.VMEM((3, D, FF), F32),
            pltpu.VMEM((FF, LW), BF),
            pltpu.VMEM((FC, LW), BF),
            pltpu.VMEM((3, 2, 128, MTOK), BF),
            pltpu.VMEM((NL, 4, 2, SH, 128), BF),
            pltpu.VMEM((NL, 4, SH, 128), BF),
            pltpu.VMEM((2, NL, 2, SH, 128), BF),
            pltpu.VMEM((NL, 2, SH, 128), BF),
            pltpu.VMEM((2, NL, SH, 128), BF),
            pltpu.VMEM((NL, SH, 128), BF),
            dma((14,)), dma((9,)), dma((4,)), dma((5,)), dma((3 * NP,)), dma((3 * NP,)), dma((4, NP)), dma((4, NP)), dma((NP,)), dma((NP,)),
        ],
        compiler_params=pltpu.CompilerParams(
            collective_id=0, has_side_effects=True, vmem_limit_bytes=40 * 1024 * 1024),
        cost_estimate=pl.CostEstimate(flops=9_000_000_000, bytes_accessed=7_000_000, transcendentals=5_000_000),
    )(*args)
    mid = [pltpu.with_memory_space_constraint(t, pltpu.VMEM) for t in mid]
    return pl.pallas_call(
        finish,
        name="mlp_bwd_finish",
        out_shape=[pltpu.HBM((2, D, MTOK), BF), pltpu.HBM((3, D, SH), F32), pltpu.HBM((1, 3, D, FF), F32)],
        in_specs=[vm] * 4,
        out_specs=[hbm] * 3,
        scratch_shapes=[
            pltpu.VMEM((3, D, SH), F32), dma((6,)),
        ],
        compiler_params=pltpu.CompilerParams(vmem_limit_bytes=16 * 1024 * 1024),
        cost_estimate=pl.CostEstimate(flops=2_000_000, bytes_accessed=5_000_000, transcendentals=0),
    )(*mid)


def solution(mesh):
    def local_step(x_dev, dy_dev, gate_shard, up_shard, down_shard, g_dev):
        dx_t, grad_next, grad_layer = fused(
            jnp.swapaxes(x_dev, 1, 2), jnp.swapaxes(dy_dev, 1, 2), gate_shard, up_shard, down_shard, g_dev)
        return jnp.swapaxes(dx_t, 1, 2), grad_next, grad_layer

    in_specs = (P(None, TOK_AXES, None), P(None, TOK_AXES, None), P(None, GROUP_AXES), P(None, GROUP_AXES), P(GROUP_AXES, None), P(TOK_AXES, None, None, None))
    out_specs = (P(None, TOK_AXES, None), P(None, None, GROUP_AXES), P(TOK_AXES, None, None, None))
    return jax.shard_map(local_step, mesh=mesh, in_specs=in_specs, out_specs=out_specs, check_vma=False)
```

```python
import functools
import jax
import jax.numpy as jnp
from jax import lax
from jax.experimental import pallas as pl
from jax.experimental.pallas import tpu as pltpu
from jax.sharding import PartitionSpec as P

TOK_AXES = ("dp", "row", "fsdp")
GROUP_AXES = ("row", "fsdp")
MESH = pl.DeviceIdType.MESH
BF = jnp.bfloat16
F32 = jnp.float32

D = 288
FF = 768
SH = 96
LW = 896
FC = 256
TT = 256
MTOK = 1536
PIECES = ((0, 2), (2, 4), (4, 7))
NP = len(PIECES)
SUMMED = (0, 1)
NL = LW // 128
NT_DIMS = (((1,), (1,)), ((), ()))
CUTS = tuple(
    (b, lo - FC * b, sh, lo - SH * sh, hi - lo)
    for b in range(FF // FC) for sh in range(FF // SH)
    for lo, hi in [(max(FC * b, SH * sh), min(FC * b + FC, SH * sh + SH))] if lo < hi
)


def dot(a, b):
    return jnp.dot(a, b, preferred_element_type=F32)


def dot_nt(a, b):
    return lax.dot_general(a, b, NT_DIMS, preferred_element_type=F32)


def eye(n):
    r = lax.broadcasted_iota(jnp.int32, (n, n), 0)
    c = lax.broadcasted_iota(jnp.int32, (n, n), 1)
    return (r == c).astype(F32).astype(BF)


PRE = ("send_p", "send_64", "send_y.0", "send_y.1", "g.0", "g.1", "g.2", "send_x.0", "send_x.1", "tails", "own_p",)
EVENTS = {
    2: ("pair.0", "pair.1", "pair.2",),
    9: ("pass64",),
    11: ("x64",),
    23: ("ph1.0", "ph1.1", "y",),
    27: ("xrest", "ph1.2",),
    30: ("ph2.0", "ph2.1", "rest2",),
    36: ("ph2.2",),
    42: ("diag", "relay.0",),
    49: ("rest3", "relay.1",),
    55: ("relay.2",),
    68: ("zall.0", "zall.1", "zall.2",),
}


def body(x_hbm, dy_hbm, wg_hbm, wu_hbm, wd_hbm, g_hbm,
         dx_ref, dw_ref, zb, tot,
         xt, yt, hh, wn, dxacc, wg, wu, wd, g32, wire, wc, xtail,
         gt, gr, s1, r1, s2, r2,
         in_sem, ws_sem, wrd_sem, wrp_sem, gs_sem, gr_sem, zs_sem, zr_sem, ts_sem, tr_sem):
    z = lax.axis_index("dp")
    y = lax.axis_index("row")
    f = lax.axis_index("fsdp")
    x = f // 2
    c = f % 2
    ny = 1 - y
    partner = (z, y, f + 1 - 2 * c)
    nbr_x = (z, y, (f + 2) % 4)
    nbr_y = (z, ny, f)
    nbr_a = (z, y + (1 - c) * (1 - 2 * y), (f + 2 * c) % 4)
    nbr_b = (z, y + c * (1 - 2 * y), (f + 2 * (1 - c)) % 4)
    ax_a = 1 - c
    ax_b = c
    split = c == 1 - x
    gets = c == x

    g_loads = [pltpu.make_async_copy(g_hbm.at[0, k], g32.at[k], in_sem.at[k]) for k in range(3)]
    w_loads = [
        pltpu.make_async_copy(wg_hbm, wg, in_sem.at[9]),
        pltpu.make_async_copy(wu_hbm, wu, in_sem.at[10]),
        pltpu.make_async_copy(wd_hbm, wd, in_sem.at[11]),
    ]
    x_loads = [
        pltpu.make_async_copy(x_hbm, xt, in_sem.at[12]),
        pltpu.make_async_copy(dy_hbm, yt, in_sem.at[13]),
    ]
    for l in w_loads + g_loads + x_loads:
        l.start()

    bar = pltpu.get_barrier_semaphore()
    for dev in (partner, nbr_a, nbr_b):
        pl.semaphore_signal(bar, inc=1, device_id=dev, device_id_type=MESH)

    mid = jnp.logical_or(z == 1, z == 2)
    end = jnp.logical_not(mid)
    near = jnp.where(z == 0, 1, jnp.where(z == 3, 2, 3 - z))
    far = jnp.where(z == 0, 2, jnp.where(z == 3, 1, jnp.where(z == 1, 3, 0)))
    mine = jnp.where(z == 1, 0, 3)

    pl.semaphore_signal(bar, inc=1, device_id=(near, y, f), device_id_type=MESH)
    pl.semaphore_signal(bar, inc=1, device_id=(far, y, f), device_id_type=MESH)

    @pl.when(mid)
    def _():
        pl.semaphore_signal(bar, inc=1, device_id=(mine, y, f), device_id_type=MESH)

    def ds(start, n):
        return pl.ds(pl.multiple_of(start, 32), n)

    def rows_of(yy, xx, cc):
        return ds((4 * yy + 2 * xx + cc) * SH, SH)

    own = rows_of(y, x, c)
    i96 = eye(SH)
    for l in w_loads:
        l.wait()
    wire[own, 0:256] = dot_nt(i96, wg[0:256, :]).astype(BF)
    wire[own, 256:512] = dot_nt(i96, wu[0:256, :]).astype(BF)
    wire[own, 512:768] = wd[:, 0:256]
    tails = dot_nt(i96, jnp.concatenate([wg[256:288, :], wu[256:288, :]], 0)).astype(BF)
    wire[own, 768:896] = jnp.concatenate([tails, wd[:, 256:288], jnp.zeros((SH, 32), BF)], 1)

    @pl.when(mid)
    def _():
        pl.semaphore_wait(bar, 6)

    @pl.when(end)
    def _():
        pl.semaphore_wait(bar, 5)

    def remote(src, dst, ssem, rsem, dev):
        return pltpu.make_async_remote_copy(src_ref=src, dst_ref=dst, send_sem=ssem, recv_sem=rsem,
                                            device_id=dev, device_id_type=MESH)

    def wcopy(rows, send, recv, dev):
        return remote(wire.at[rows], wire.at[rows], ws_sem.at[send], recv, dev)

    def wrecv(rows, sem):
        wcopy(rows, 0, sem, partner).wait_recv()

    def r64(xs):
        return ds(384 * y + 128 + 64 * xs, 64)

    def r32(xs):
        return ds(384 * y + 96 + 160 * xs, 32)

    sends = []

    def start(cp, cond=None):
        sends.append((cp, cond))
        if cond is None:
            cp.start()
        else:
            @pl.when(cond)
            def _():
                cp.start()

    def ev_send_p():
        start(wcopy(own, 1, wrp_sem.at[0], partner))

    def ev_send_64():
        start(wcopy(r64(x), 0, wrd_sem.at[0], nbr_x), split)

    def ev_send_y(core):
        start(wcopy(own, 2, wrd_sem.at[2], nbr_y), c == core)

    def ev_send_x(part):
        if part == 0:
            start(wcopy(r32(x), 3, wrd_sem.at[1], nbr_x), split)
        else:
            start(wcopy(own, 3, wrd_sem.at[1], nbr_x), jnp.logical_not(split))

    i256 = eye(256)

    def pair_copy(p):
        lo, hi = PIECES[p]
        return remote(gt.at[lo:hi, :, 1 - c], gr.at[lo:hi], gs_sem.at[p], gr_sem.at[p], partner)

    def put(o, fb, t):
        for blk, r0, sh, r, m in CUTS:
            if blk == fb:
                gt[t, sh // 2, sh % 2, r:r + m, :] = o[r0:r0 + m]

    def ready(*tiles):
        for p in range(NP):
            if PIECES[p][1] - 1 in tiles:
                start(pair_copy(p))

    def ev_g(k):
        g_loads[k].wait()
        for fb in range(3):
            o = dot_nt(i256, g32[k, 0:256, 256 * fb:256 * fb + 256].astype(BF)).astype(BF)
            put(o[:, 0:128], fb, 2 * k)
            put(o[:, 128:256], fb, 2 * k + 1)
        if k == 2:
            for fb in range(3):
                tl = jnp.concatenate([g32[j, 256:288, 256 * fb:256 * fb + 256].astype(BF) for j in range(3)]
                                     + [jnp.zeros((32, 256), BF)], 0)
                put(dot_nt(i256, tl).astype(BF), fb, 6)
        ready(*((2 * k, 2 * k + 1) if k < 2 else (4, 5, 6)))

    def ev_tails():
        for l in x_loads:
            l.wait()
        for m in range(2):
            xtl = xt[m, 256:288]
            xtail[0, m] = jnp.concatenate([xtl, jnp.zeros((96, MTOK), BF)], 0)
            xtail[1, m] = jnp.concatenate([jnp.zeros((32, MTOK), BF), xtl, jnp.zeros((64, MTOK), BF)], 0)
            xtail[2, m] = jnp.concatenate([jnp.zeros((64, MTOK), BF), yt[m, 256:288], jnp.zeros((32, MTOK), BF)], 0)

    def chip(ra, rb):
        ya_ = y + (1 - 2 * y) * (ra * ax_a + rb * ax_b)
        xa_ = x + (1 - 2 * x) * (ra * ax_b + rb * ax_a)
        return 2 * ya_ + xa_

    def add(p, q):
        return (p.astype(F32) + q.astype(F32)).astype(BF)

    def ph1(p):
        lo, hi = PIECES[p]
        return remote(s1.at[1, lo:hi], r1.at[lo:hi], gs_sem.at[NP + p], gr_sem.at[NP + p], nbr_a)

    def ph2(p):
        lo, hi = PIECES[p]
        return remote(s2.at[1, lo:hi], r2.at[lo:hi], gs_sem.at[2 * NP + p], gr_sem.at[2 * NP + p], nbr_b)

    def zcopy(slot, p, send, dev):
        lo, hi = PIECES[p]
        return remote(zb.at[slot, lo:hi], zb.at[slot, lo:hi], zs_sem.at[send, p], zr_sem.at[slot, p], (dev, y, f))

    def ev_pair(p):
        lo, hi = PIECES[p]
        pair_copy(p).wait_recv()
        for ra in (1, 0):
            for rb in range(2):
                q = chip(ra, rb)
                s1[ra, lo:hi, rb] = add(gt[lo:hi, q, c], gr[lo:hi, q])
            if ra == 1:
                start(ph1(p))

    def ev_ph1(p):
        lo, hi = PIECES[p]
        ph1(p).wait_recv()
        s2[1, lo:hi] = add(s1[0, lo:hi, 1], r1[lo:hi, 1])
        start(ph2(p))
        s2[0, lo:hi] = add(s1[0, lo:hi, 0], r1[lo:hi, 0])

    def ev_ph2(p):
        lo, hi = PIECES[p]
        ph2(p).wait_recv()
        zb[z, lo:hi] = add(s2[0, lo:hi], r2[lo:hi])
        if p in SUMMED:
            start(zcopy(z, p, 1, far), end)
            start(zcopy(z, p, 0, near))
        else:
            start(zcopy(z, p, 1, far))
            start(zcopy(z, p, 0, near))
            start(zcopy(z, p, 2, mine), mid)

    def tcopy(p):
        lo, hi = PIECES[p]
        return remote(tot.at[lo:hi], tot.at[lo:hi], ts_sem.at[p], tr_sem.at[p], (mine, y, f))

    def ev_relay(p):
        @pl.when(mid)
        def _():
            zcopy(far, p, 0, near).wait_recv()
        if p in SUMMED:
            lo, hi = PIECES[p]

            @pl.when(mid)
            def _():
                zcopy(near, p, 0, near).wait_recv()
                zcopy(mine, p, 0, near).wait_recv()
                tot[lo:hi] = z_sum(zb, lo, hi)
            start(tcopy(p), mid)
        else:
            start(zcopy(far, p, 3, mine), mid)

    def ev_zall(p):
        if p in SUMMED:
            @pl.when(end)
            def _():
                tcopy(p).wait_recv()
        else:
            zcopy(near, p, 0, near).wait_recv()

            @pl.when(mid)
            def _():
                zcopy(mine, p, 0, near).wait_recv()

            @pl.when(end)
            def _():
                zcopy(far, p, 0, near).wait_recv()
                zcopy(3 - z, p, 0, near).wait_recv()

    def ev_own_p():
        wrecv(rows_of(y, x, 1 - c), wrp_sem.at[0])

    def ev_pass64():
        @pl.when(gets)
        def _():
            wrecv(r64(1 - x), wrd_sem.at[0])
        start(wcopy(r64(1 - x), 4, wrp_sem.at[1], partner), gets)

    def ev_x64():
        @pl.when(jnp.logical_not(gets))
        def _():
            wrecv(r64(1 - x), wrp_sem.at[1])

    def ev_xrest():
        @pl.when(gets)
        def _():
            wrecv(r32(1 - x), wrd_sem.at[1])

        @pl.when(jnp.logical_not(gets))
        def _():
            wrecv(rows_of(y, 1 - x, c), wrd_sem.at[1])
        start(wcopy(r32(1 - x), 5, wrp_sem.at[2], partner), gets)
        start(wcopy(rows_of(y, 1 - x, c), 5, wrp_sem.at[2], partner), jnp.logical_not(gets))
        start(wcopy(rows_of(y, 1 - x, c), 6, wrd_sem.at[3], nbr_y), c == 1)

    def ev_y():
        wrecv(rows_of(ny, x, c), wrd_sem.at[2])
        start(wcopy(rows_of(ny, x, c), 7, wrp_sem.at[3], partner))
        start(wcopy(rows_of(ny, x, c), 6, wrd_sem.at[3], nbr_x), c == 0)

    def ev_diag():
        wrecv(rows_of(ny, 1 - x, c), wrd_sem.at[3])
        start(wcopy(rows_of(ny, 1 - x, c), 8, wrp_sem.at[4], partner))

    def ev_rest2():
        @pl.when(gets)
        def _():
            wrecv(rows_of(y, 1 - x, 1 - c), wrp_sem.at[2])

        @pl.when(jnp.logical_not(gets))
        def _():
            wrecv(r32(1 - x), wrp_sem.at[2])
        wrecv(rows_of(ny, x, 1 - c), wrp_sem.at[3])

    def ev_rest3():
        wrecv(rows_of(ny, 1 - x, 1 - c), wrp_sem.at[4])

    handlers = {
        "pair": ev_pair, "ph1": ev_ph1, "ph2": ev_ph2, "relay": ev_relay, "zall": ev_zall, "g": ev_g, "tails": ev_tails, "send_p": ev_send_p, "send_64": ev_send_64, "send_y": ev_send_y, "send_x": ev_send_x, "own_p": ev_own_p, "x64": ev_x64, "pass64": ev_pass64,
        "xrest": ev_xrest, "y": ev_y, "diag": ev_diag, "rest2": ev_rest2, "rest3": ev_rest3,
    }

    ticks = [0]

    def run(evs):
        for ev in evs:
            name, _, arg = ev.partition(".")
            with jax.named_scope(ev.replace(".", "_")):
                handlers[name](*([int(arg)] if arg else []))

    def tick():
        run(EVENTS.get(ticks[0], ()))
        ticks[0] += 1

    def forward(w, rows, h0, n):
        for m in range(2):
            for t in range(MTOK // TT):
                forward_step(w, rows, h0, n, m, slice(t * TT, t * TT + TT))
                tick()

    def forward_step(w, rows, h0, n, m, col):
        tl = w[rows, 768:896]
        xm = xt[m, 0:256, col]
        a = dot(w[rows, 0:256], xm) + dot(tl, xtail[0, m, :, col])
        b = dot(w[rows, 256:512], xm) + dot(tl, xtail[1, m, :, col])
        dh = dot(w[rows, 512:768], yt[m, 0:256, col]) + dot(tl, xtail[2, m, :, col])
        s = 1.0 / (1.0 + jnp.exp(-a))
        act = a * s
        hh[m, ds(h0, n), col] = (dh * b * (s + act * (1.0 - s))).astype(BF)
        hh[m, ds(FC + h0, n), col] = (dh * act).astype(BF)
        hh[m, ds(2 * FC + h0, n), col] = (act * b).astype(BF)

    def natural(w, rows):
        t = dot_nt(i256[:128, :128], w[rows, 768:896]).astype(BF)
        for k in range(2):
            wn[0:256, k * FC:k * FC + FC] = dot_nt(i256, w[rows, 256 * k:256 * k + 256]).astype(BF)
            wn[256:288, k * FC:k * FC + FC] = t[32 * k:32 * k + 32]

    def backward(j, lanes):
        for m in range(2):
            for n in range(2):
                col = slice(768 * n, 768 * n + 768)
                d = dot(wn[...], hh[m, 0:2 * FC, col])
                if j == 1:
                    dxacc[m, :, col] = d
                elif j == 2:
                    dxacc[m, :, col] = d + dxacc[m, :, col]
                else:
                    dx_ref[m, :, col] = (d + dxacc[m, :, col]).astype(BF)
                tick()
        for k in range(3):
            o = grad_w(k, xt, yt, hh)
            for i, l in enumerate(lanes):
                dw_ref[0, k, :, lane_tile(l)] = o[:, 128 * i:128 * i + 128]
            tick()

    run(PRE)
    forward(wire, ds(384 * y + 192 * x, 192), 64 * x, 192)
    forward(wire, r64(1 - x), 192 * (1 - x), 64)
    first = 384 * y + 128 * x
    natural(wire, ds(first, FC))
    backward(1, (first, first + 128))

    second = (384 * y + 256 - 256 * x, 384 * ny + 256 * x)
    for i, l in enumerate(second):
        wc[128 * i:128 * i + 128] = wire[ds(l, 128)]
    full = slice(0, FC)
    forward(wc, full, 0, FC)
    natural(wc, full)
    backward(2, second)

    third = 384 * ny + 128 * (1 - x)
    forward(wire, ds(third, FC), 0, FC)
    natural(wire, ds(third, FC))
    backward(3, (third, third + 128))
    assert max(EVENTS) < ticks[0]

    for cp, cond in sends:
        if cond is None:
            cp.wait_send()
        else:
            @pl.when(cond)
            def _():
                cp.wait_send()


def lane_tile(l):
    return pl.ds(pl.multiple_of(l, 128), 128)


def grad_w(k, xt, yt, hh):
    t = yt if k == 2 else xt
    hk = slice(k * FC, k * FC + FC)
    return dot_nt(t[0], hh[0, hk]) + dot_nt(t[1], hh[1, hk])


def z_sum(zb, lo, hi):
    t = zb[0, lo:hi].astype(F32) + zb[1, lo:hi].astype(F32)
    t = t + zb[2, lo:hi].astype(F32)
    return t + zb[3, lo:hi].astype(F32)


def finish(dx, dw, zb, tot, dx_hbm, gn_hbm, dw_hbm, gno, sem):
    copies = [pltpu.make_async_copy(dw.at[0, k], dw_hbm.at[0, k], sem.at[k]) for k in range(3)]
    copies += [pltpu.make_async_copy(dx.at[m], dx_hbm.at[m], sem.at[3 + m]) for m in range(2)]
    for cp in copies:
        cp.start()
    for i in range(NL):
        piece = [lo <= i < hi for lo, hi in PIECES].index(True)
        t = tot[i] if piece in SUMMED else z_sum(zb, i, i + 1)[0]
        t = jnp.concatenate([t, jnp.zeros((32, 128), F32)], 0).T[:, 0:SH]
        if i < 6:
            gno[i // 2, 128 * (i % 2):128 * (i % 2) + 128, :] = t
        else:
            for s in range(3):
                gno[s, 256:288, :] = t[32 * s:32 * s + 32]
    copies.append(pltpu.make_async_copy(gno, gn_hbm, sem.at[5]))
    copies[-1].start()
    for cp in copies:
        cp.wait()


def fused(x_t, dy_t, wg, wu, wd, g):
    hbm = pl.BlockSpec(memory_space=pltpu.HBM)
    vm = pl.BlockSpec(memory_space=pltpu.VMEM)
    dma = pltpu.SemaphoreType.DMA
    state = [pltpu.VMEM((2, D, MTOK), BF), pltpu.VMEM((1, 3, D, FF), F32), pltpu.VMEM((4, NL, SH, 128), BF), pltpu.VMEM((NL, SH, 128), F32)]
    args = [pltpu.with_memory_space_constraint(t, pltpu.HBM) for t in (x_t, dy_t, wg, wu, wd, g)]
    mid = pl.pallas_call(
        body,
        name="mlp_bwd",
        out_shape=state,
        in_specs=[hbm] * 6,
        out_specs=[vm] * 4,
        scratch_shapes=[
            pltpu.VMEM((2, D, MTOK), BF), pltpu.VMEM((2, D, MTOK), BF),
            pltpu.VMEM((2, 3 * FC, MTOK), BF),
            pltpu.VMEM((D, 2 * FC), BF),
            pltpu.VMEM((2, D, MTOK), F32),
            pltpu.VMEM((D, SH), BF), pltpu.VMEM((D, SH), BF), pltpu.VMEM((SH, D), BF),
            pltpu.VMEM((3, D, FF), F32),
            pltpu.VMEM((FF, LW), BF),
            pltpu.VMEM((FC, LW), BF),
            pltpu.VMEM((3, 2, 128, MTOK), BF),
            pltpu.VMEM((NL, 4, 2, SH, 128), BF),
            pltpu.VMEM((NL, 4, SH, 128), BF),
            pltpu.VMEM((2, NL, 2, SH, 128), BF),
            pltpu.VMEM((NL, 2, SH, 128), BF),
            pltpu.VMEM((2, NL, SH, 128), BF),
            pltpu.VMEM((NL, SH, 128), BF),
            dma((14,)), dma((9,)), dma((4,)), dma((5,)), dma((3 * NP,)), dma((3 * NP,)), dma((4, NP)), dma((4, NP)), dma((NP,)), dma((NP,)),
        ],
        compiler_params=pltpu.CompilerParams(
            collective_id=0, has_side_effects=True, vmem_limit_bytes=40 * 1024 * 1024),
        cost_estimate=pl.CostEstimate(flops=9_000_000_000, bytes_accessed=7_000_000, transcendentals=5_000_000),
    )(*args)
    mid = [pltpu.with_memory_space_constraint(t, pltpu.VMEM) for t in mid]
    return pl.pallas_call(
        finish,
        name="mlp_bwd_finish",
        out_shape=[pltpu.HBM((2, D, MTOK), BF), pltpu.HBM((3, D, SH), F32), pltpu.HBM((1, 3, D, FF), F32)],
        in_specs=[vm] * 4,
        out_specs=[hbm] * 3,
        scratch_shapes=[
            pltpu.VMEM((3, D, SH), F32), dma((6,)),
        ],
        compiler_params=pltpu.CompilerParams(vmem_limit_bytes=16 * 1024 * 1024),
        cost_estimate=pl.CostEstimate(flops=2_000_000, bytes_accessed=5_000_000, transcendentals=0),
    )(*mid)


def solution(mesh):
    def local_step(x_dev, dy_dev, gate_shard, up_shard, down_shard, g_dev):
        dx_t, grad_next, grad_layer = fused(
            jnp.swapaxes(x_dev, 1, 2), jnp.swapaxes(dy_dev, 1, 2), gate_shard, up_shard, down_shard, g_dev)
        return jnp.swapaxes(dx_t, 1, 2), grad_next, grad_layer

    in_specs = (P(None, TOK_AXES, None), P(None, TOK_AXES, None), P(None, GROUP_AXES), P(None, GROUP_AXES), P(GROUP_AXES, None), P(TOK_AXES, None, None, None))
    out_specs = (P(None, TOK_AXES, None), P(None, None, GROUP_AXES), P(TOK_AXES, None, None, None))
    return jax.shard_map(local_step, mesh=mesh, in_specs=in_specs, out_specs=out_specs, check_vma=False)
```

```python
import functools
import jax
import jax.numpy as jnp
from jax import lax
from jax.experimental import pallas as pl
from jax.experimental.pallas import tpu as pltpu
from jax.sharding import PartitionSpec as P

TOK_AXES = ("dp", "row", "fsdp")
GROUP_AXES = ("row", "fsdp")
MESH = pl.DeviceIdType.MESH
BF = jnp.bfloat16
F32 = jnp.float32

D = 288
FF = 768
SH = 96
LW = 896
FC = 256
TT = 256
MTOK = 1536
PIECES = ((0, 2), (2, 4), (4, 7))
NP = len(PIECES)
SUMMED = (0, 1)
NL = LW // 128
NT_DIMS = (((1,), (1,)), ((), ()))
CUTS = tuple(
    (b, lo - FC * b, sh, lo - SH * sh, hi - lo)
    for b in range(FF // FC) for sh in range(FF // SH)
    for lo, hi in [(max(FC * b, SH * sh), min(FC * b + FC, SH * sh + SH))] if lo < hi
)


def dot(a, b):
    return jnp.dot(a, b, preferred_element_type=F32)


def dot_nt(a, b):
    return lax.dot_general(a, b, NT_DIMS, preferred_element_type=F32)


def eye(n):
    r = lax.broadcasted_iota(jnp.int32, (n, n), 0)
    c = lax.broadcasted_iota(jnp.int32, (n, n), 1)
    return (r == c).astype(F32).astype(BF)


PRE = ("send_p", "send_64", "send_y.0", "send_y.1", "g.0", "g.1", "g.2", "send_x.0", "send_x.1", "tails", "own_p",)
EVENTS = {
    2: ("pair.0", "pair.1", "pair.2",),
    9: ("pass64",),
    11: ("x64",),
    23: ("ph1.0", "ph1.1", "y",),
    27: ("xrest", "ph1.2",),
    30: ("ph2.0", "ph2.1", "rest2",),
    36: ("ph2.2",),
    42: ("diag", "relay.0",),
    49: ("rest3", "relay.1",),
    55: ("relay.2",),
    68: ("zall.0", "zall.1", "zall.2",),
}


def body(x_hbm, dy_hbm, wg_hbm, wu_hbm, wd_hbm, g_hbm,
         dx_ref, dw_ref, zb, tot,
         xt, yt, hh, wn, dxacc, wg, wu, wd, g32, wire, wc, xtail,
         gt, gr, s1, r1, s2, r2,
         in_sem, ws_sem, wrd_sem, wrp_sem, gs_sem, gr_sem, zs_sem, zr_sem, ts_sem, tr_sem):
    z = lax.axis_index("dp")
    y = lax.axis_index("row")
    f = lax.axis_index("fsdp")
    x = f // 2
    c = f % 2
    ny = 1 - y
    partner = (z, y, f + 1 - 2 * c)
    nbr_x = (z, y, (f + 2) % 4)
    nbr_y = (z, ny, f)
    nbr_a = (z, y + (1 - c) * (1 - 2 * y), (f + 2 * c) % 4)
    nbr_b = (z, y + c * (1 - 2 * y), (f + 2 * (1 - c)) % 4)
    ax_a = 1 - c
    ax_b = c
    split = c == 1 - x
    gets = c == x

    g_loads = [pltpu.make_async_copy(g_hbm.at[0, k], g32.at[k], in_sem.at[k]) for k in range(3)]
    w_loads = [
        pltpu.make_async_copy(wg_hbm, wg, in_sem.at[9]),
        pltpu.make_async_copy(wu_hbm, wu, in_sem.at[10]),
        pltpu.make_async_copy(wd_hbm, wd, in_sem.at[11]),
    ]
    x_loads = [
        pltpu.make_async_copy(x_hbm, xt, in_sem.at[12]),
        pltpu.make_async_copy(dy_hbm, yt, in_sem.at[13]),
    ]
    for l in w_loads + g_loads + x_loads:
        l.start()

    bar = pltpu.get_barrier_semaphore()
    for dev in (partner, nbr_a, nbr_b):
        pl.semaphore_signal(bar, inc=1, device_id=dev, device_id_type=MESH)

    mid = jnp.logical_or(z == 1, z == 2)
    end = jnp.logical_not(mid)
    near = jnp.where(z == 0, 1, jnp.where(z == 3, 2, 3 - z))
    far = jnp.where(z == 0, 2, jnp.where(z == 3, 1, jnp.where(z == 1, 3, 0)))
    mine = jnp.where(z == 1, 0, 3)

    pl.semaphore_signal(bar, inc=1, device_id=(near, y, f), device_id_type=MESH)
    pl.semaphore_signal(bar, inc=1, device_id=(far, y, f), device_id_type=MESH)

    @pl.when(mid)
    def _():
        pl.semaphore_signal(bar, inc=1, device_id=(mine, y, f), device_id_type=MESH)

    def ds(start, n):
        return pl.ds(pl.multiple_of(start, 32), n)

    def rows_of(yy, xx, cc):
        return ds((4 * yy + 2 * xx + cc) * SH, SH)

    own = rows_of(y, x, c)
    i96 = eye(SH)
    for l in w_loads:
        l.wait()
    wire[own, 0:256] = dot_nt(i96, wg[0:256, :]).astype(BF)
    wire[own, 256:512] = dot_nt(i96, wu[0:256, :]).astype(BF)
    wire[own, 512:768] = wd[:, 0:256]
    tails = dot_nt(i96, jnp.concatenate([wg[256:288, :], wu[256:288, :]], 0)).astype(BF)
    wire[own, 768:896] = jnp.concatenate([tails, wd[:, 256:288], jnp.zeros((SH, 32), BF)], 1)

    @pl.when(mid)
    def _():
        pl.semaphore_wait(bar, 6)

    @pl.when(end)
    def _():
        pl.semaphore_wait(bar, 5)

    def remote(src, dst, ssem, rsem, dev):
        return pltpu.make_async_remote_copy(src_ref=src, dst_ref=dst, send_sem=ssem, recv_sem=rsem,
                                            device_id=dev, device_id_type=MESH)

    def wcopy(rows, send, recv, dev):
        return remote(wire.at[rows], wire.at[rows], ws_sem.at[send], recv, dev)

    def wrecv(rows, sem):
        wcopy(rows, 0, sem, partner).wait_recv()

    def r64(xs):
        return ds(384 * y + 128 + 64 * xs, 64)

    def r32(xs):
        return ds(384 * y + 96 + 160 * xs, 32)

    sends = []

    def start(cp, cond=None):
        sends.append((cp, cond))
        if cond is None:
            cp.start()
        else:
            @pl.when(cond)
            def _():
                cp.start()

    def ev_send_p():
        start(wcopy(own, 1, wrp_sem.at[0], partner))

    def ev_send_64():
        start(wcopy(r64(x), 0, wrd_sem.at[0], nbr_x), split)

    def ev_send_y(core):
        start(wcopy(own, 2, wrd_sem.at[2], nbr_y), c == core)

    def ev_send_x(part):
        if part == 0:
            start(wcopy(r32(x), 3, wrd_sem.at[1], nbr_x), split)
        else:
            start(wcopy(own, 3, wrd_sem.at[1], nbr_x), jnp.logical_not(split))

    i256 = eye(256)

    def pair_copy(p):
        lo, hi = PIECES[p]
        return remote(gt.at[lo:hi, :, 1 - c], gr.at[lo:hi], gs_sem.at[p], gr_sem.at[p], partner)

    def put(o, fb, t):
        for blk, r0, sh, r, m in CUTS:
            if blk == fb:
                gt[t, sh // 2, sh % 2, r:r + m, :] = o[r0:r0 + m]

    def ready(*tiles):
        for p in range(NP):
            if PIECES[p][1] - 1 in tiles:
                start(pair_copy(p))

    def ev_g(k):
        g_loads[k].wait()
        for fb in range(3):
            o = dot_nt(i256, g32[k, 0:256, 256 * fb:256 * fb + 256].astype(BF)).astype(BF)
            put(o[:, 0:128], fb, 2 * k)
            put(o[:, 128:256], fb, 2 * k + 1)
        if k == 2:
            for fb in range(3):
                tl = jnp.concatenate([g32[j, 256:288, 256 * fb:256 * fb + 256].astype(BF) for j in range(3)]
                                     + [jnp.zeros((32, 256), BF)], 0)
                put(dot_nt(i256, tl).astype(BF), fb, 6)
        ready(*((2 * k, 2 * k + 1) if k < 2 else (4, 5, 6)))

    def ev_tails():
        for l in x_loads:
            l.wait()
        for m in range(2):
            xtl = xt[m, 256:288]
            xtail[0, m] = jnp.concatenate([xtl, jnp.zeros((96, MTOK), BF)], 0)
            xtail[1, m] = jnp.concatenate([jnp.zeros((32, MTOK), BF), xtl, jnp.zeros((64, MTOK), BF)], 0)
            xtail[2, m] = jnp.concatenate([jnp.zeros((64, MTOK), BF), yt[m, 256:288], jnp.zeros((32, MTOK), BF)], 0)

    def chip(ra, rb):
        ya_ = y + (1 - 2 * y) * (ra * ax_a + rb * ax_b)
        xa_ = x + (1 - 2 * x) * (ra * ax_b + rb * ax_a)
        return 2 * ya_ + xa_

    def add(p, q):
        return (p.astype(F32) + q.astype(F32)).astype(BF)

    def ph1(p):
        lo, hi = PIECES[p]
        return remote(s1.at[1, lo:hi], r1.at[lo:hi], gs_sem.at[NP + p], gr_sem.at[NP + p], nbr_a)

    def ph2(p):
        lo, hi = PIECES[p]
        return remote(s2.at[1, lo:hi], r2.at[lo:hi], gs_sem.at[2 * NP + p], gr_sem.at[2 * NP + p], nbr_b)

    def zcopy(slot, p, send, dev):
        lo, hi = PIECES[p]
        return remote(zb.at[slot, lo:hi], zb.at[slot, lo:hi], zs_sem.at[send, p], zr_sem.at[slot, p], (dev, y, f))

    def ev_pair(p):
        lo, hi = PIECES[p]
        pair_copy(p).wait_recv()
        for ra in (1, 0):
            for rb in range(2):
                q = chip(ra, rb)
                s1[ra, lo:hi, rb] = add(gt[lo:hi, q, c], gr[lo:hi, q])
            if ra == 1:
                start(ph1(p))

    def ev_ph1(p):
        lo, hi = PIECES[p]
        ph1(p).wait_recv()
        s2[1, lo:hi] = add(s1[0, lo:hi, 1], r1[lo:hi, 1])
        start(ph2(p))
        s2[0, lo:hi] = add(s1[0, lo:hi, 0], r1[lo:hi, 0])

    def ev_ph2(p):
        lo, hi = PIECES[p]
        ph2(p).wait_recv()
        zb[z, lo:hi] = add(s2[0, lo:hi], r2[lo:hi])
        if p in SUMMED:
            start(zcopy(z, p, 1, far), end)
            start(zcopy(z, p, 0, near))
        else:
            start(zcopy(z, p, 1, far))
            start(zcopy(z, p, 0, near))
            start(zcopy(z, p, 2, mine), mid)

    def tcopy(p):
        lo, hi = PIECES[p]
        return remote(tot.at[lo:hi], tot.at[lo:hi], ts_sem.at[p], tr_sem.at[p], (mine, y, f))

    def ev_relay(p):
        @pl.when(mid)
        def _():
            zcopy(far, p, 0, near).wait_recv()
        if p in SUMMED:
            lo, hi = PIECES[p]

            @pl.when(mid)
            def _():
                zcopy(near, p, 0, near).wait_recv()
                zcopy(mine, p, 0, near).wait_recv()
                tot[lo:hi] = z_sum(zb, lo, hi)
            start(tcopy(p), mid)
        else:
            start(zcopy(far, p, 3, mine), mid)

    def ev_zall(p):
        if p in SUMMED:
            @pl.when(end)
            def _():
                tcopy(p).wait_recv()
        else:
            zcopy(near, p, 0, near).wait_recv()

            @pl.when(mid)
            def _():
                zcopy(mine, p, 0, near).wait_recv()

            @pl.when(end)
            def _():
                zcopy(far, p, 0, near).wait_recv()
                zcopy(3 - z, p, 0, near).wait_recv()

    def ev_own_p():
        wrecv(rows_of(y, x, 1 - c), wrp_sem.at[0])

    def ev_pass64():
        @pl.when(gets)
        def _():
            wrecv(r64(1 - x), wrd_sem.at[0])
        start(wcopy(r64(1 - x), 4, wrp_sem.at[1], partner), gets)

    def ev_x64():
        @pl.when(jnp.logical_not(gets))
        def _():
            wrecv(r64(1 - x), wrp_sem.at[1])

    def ev_xrest():
        @pl.when(gets)
        def _():
            wrecv(r32(1 - x), wrd_sem.at[1])

        @pl.when(jnp.logical_not(gets))
        def _():
            wrecv(rows_of(y, 1 - x, c), wrd_sem.at[1])
        start(wcopy(r32(1 - x), 5, wrp_sem.at[2], partner), gets)
        start(wcopy(rows_of(y, 1 - x, c), 5, wrp_sem.at[2], partner), jnp.logical_not(gets))
        start(wcopy(rows_of(y, 1 - x, c), 6, wrd_sem.at[3], nbr_y), c == 1)

    def ev_y():
        wrecv(rows_of(ny, x, c), wrd_sem.at[2])
        start(wcopy(rows_of(ny, x, c), 7, wrp_sem.at[3], partner))
        start(wcopy(rows_of(ny, x, c), 6, wrd_sem.at[3], nbr_x), c == 0)

    def ev_diag():
        wrecv(rows_of(ny, 1 - x, c), wrd_sem.at[3])
        start(wcopy(rows_of(ny, 1 - x, c), 8, wrp_sem.at[4], partner))

    def ev_rest2():
        @pl.when(gets)
        def _():
            wrecv(rows_of(y, 1 - x, 1 - c), wrp_sem.at[2])

        @pl.when(jnp.logical_not(gets))
        def _():
            wrecv(r32(1 - x), wrp_sem.at[2])
        wrecv(rows_of(ny, x, 1 - c), wrp_sem.at[3])

    def ev_rest3():
        wrecv(rows_of(ny, 1 - x, 1 - c), wrp_sem.at[4])

    handlers = {
        "pair": ev_pair, "ph1": ev_ph1, "ph2": ev_ph2, "relay": ev_relay, "zall": ev_zall, "g": ev_g, "tails": ev_tails, "send_p": ev_send_p, "send_64": ev_send_64, "send_y": ev_send_y, "send_x": ev_send_x, "own_p": ev_own_p, "x64": ev_x64, "pass64": ev_pass64,
        "xrest": ev_xrest, "y": ev_y, "diag": ev_diag, "rest2": ev_rest2, "rest3": ev_rest3,
    }

    ticks = [0]

    def run(evs):
        for ev in evs:
            name, _, arg = ev.partition(".")
            with jax.named_scope(ev.replace(".", "_")):
                handlers[name](*([int(arg)] if arg else []))

    def tick():
        run(EVENTS.get(ticks[0], ()))
        ticks[0] += 1

    def forward(w, rows, h0, n):
        for m in range(2):
            for t in range(MTOK // TT):
                forward_step(w, rows, h0, n, m, slice(t * TT, t * TT + TT))
                tick()

    def forward_step(w, rows, h0, n, m, col):
        tl = w[rows, 768:896]
        xm = xt[m, 0:256, col]
        if n == 64:
            ab = dot(jnp.concatenate([w[rows, 0:256], w[rows, 256:512]], 0), xm)
            a = ab[:n] + dot(tl, xtail[0, m, :, col])
            b = ab[n:] + dot(tl, xtail[1, m, :, col])
        else:
            a = dot(w[rows, 0:256], xm) + dot(tl, xtail[0, m, :, col])
            b = dot(w[rows, 256:512], xm) + dot(tl, xtail[1, m, :, col])
        dh = dot(w[rows, 512:768], yt[m, 0:256, col]) + dot(tl, xtail[2, m, :, col])
        s = 1.0 / (1.0 + jnp.exp(-a))
        act = a * s
        hh[m, ds(h0, n), col] = (dh * b * (s + act * (1.0 - s))).astype(BF)
        hh[m, ds(FC + h0, n), col] = (dh * act).astype(BF)
        hh[m, ds(2 * FC + h0, n), col] = (act * b).astype(BF)

    def natural(w, rows):
        t = dot_nt(i256[:128, :128], w[rows, 768:896]).astype(BF)
        for k in range(2):
            wn[0:256, k * FC:k * FC + FC] = dot_nt(i256, w[rows, 256 * k:256 * k + 256]).astype(BF)
            wn[256:288, k * FC:k * FC + FC] = t[32 * k:32 * k + 32]

    def backward(j, lanes):
        for m in range(2):
            for n in range(2):
                col = slice(768 * n, 768 * n + 768)
                d = dot(wn[...], hh[m, 0:2 * FC, col])
                if j == 1:
                    dxacc[m, :, col] = d
                elif j == 2:
                    dxacc[m, :, col] = d + dxacc[m, :, col]
                else:
                    dx_ref[m, :, col] = (d + dxacc[m, :, col]).astype(BF)
                tick()
        for k in range(3):
            o = grad_w(k, xt, yt, hh)
            for i, l in enumerate(lanes):
                dw_ref[0, k, :, lane_tile(l)] = o[:, 128 * i:128 * i + 128]
            tick()

    run(PRE)
    forward(wire, ds(384 * y + 192 * x, 192), 64 * x, 192)
    forward(wire, r64(1 - x), 192 * (1 - x), 64)
    first = 384 * y + 128 * x
    natural(wire, ds(first, FC))
    backward(1, (first, first + 128))

    second = (384 * y + 256 - 256 * x, 384 * ny + 256 * x)
    for i, l in enumerate(second):
        wc[128 * i:128 * i + 128] = wire[ds(l, 128)]
    full = slice(0, FC)
    forward(wc, full, 0, FC)
    natural(wc, full)
    backward(2, second)

    third = 384 * ny + 128 * (1 - x)
    forward(wire, ds(third, FC), 0, FC)
    natural(wire, ds(third, FC))
    backward(3, (third, third + 128))
    assert max(EVENTS) < ticks[0]

    for cp, cond in sends:
        if cond is None:
            cp.wait_send()
        else:
            @pl.when(cond)
            def _():
                cp.wait_send()


def lane_tile(l):
    return pl.ds(pl.multiple_of(l, 128), 128)


def grad_w(k, xt, yt, hh):
    t = yt if k == 2 else xt
    hk = slice(k * FC, k * FC + FC)
    return dot_nt(t[0], hh[0, hk]) + dot_nt(t[1], hh[1, hk])


def z_sum(zb, lo, hi):
    t = zb[0, lo:hi].astype(F32) + zb[1, lo:hi].astype(F32)
    t = t + zb[2, lo:hi].astype(F32)
    return t + zb[3, lo:hi].astype(F32)


def finish(dx, dw, zb, tot, dx_hbm, gn_hbm, dw_hbm, gno, sem):
    copies = [pltpu.make_async_copy(dw.at[0, k], dw_hbm.at[0, k], sem.at[k]) for k in range(3)]
    copies += [pltpu.make_async_copy(dx.at[m], dx_hbm.at[m], sem.at[3 + m]) for m in range(2)]
    for cp in copies:
        cp.start()
    for i in range(NL):
        piece = [lo <= i < hi for lo, hi in PIECES].index(True)
        t = tot[i] if piece in SUMMED else z_sum(zb, i, i + 1)[0]
        t = jnp.concatenate([t, jnp.zeros((32, 128), F32)], 0).T[:, 0:SH]
        if i < 6:
            gno[i // 2, 128 * (i % 2):128 * (i % 2) + 128, :] = t
        else:
            for s in range(3):
                gno[s, 256:288, :] = t[32 * s:32 * s + 32]
    copies.append(pltpu.make_async_copy(gno, gn_hbm, sem.at[5]))
    copies[-1].start()
    for cp in copies:
        cp.wait()


def fused(x_t, dy_t, wg, wu, wd, g):
    hbm = pl.BlockSpec(memory_space=pltpu.HBM)
    vm = pl.BlockSpec(memory_space=pltpu.VMEM)
    dma = pltpu.SemaphoreType.DMA
    state = [pltpu.VMEM((2, D, MTOK), BF), pltpu.VMEM((1, 3, D, FF), F32), pltpu.VMEM((4, NL, SH, 128), BF), pltpu.VMEM((NL, SH, 128), F32)]
    args = [pltpu.with_memory_space_constraint(t, pltpu.HBM) for t in (x_t, dy_t, wg, wu, wd, g)]
    mid = pl.pallas_call(
        body,
        name="mlp_bwd",
        out_shape=state,
        in_specs=[hbm] * 6,
        out_specs=[vm] * 4,
        scratch_shapes=[
            pltpu.VMEM((2, D, MTOK), BF), pltpu.VMEM((2, D, MTOK), BF),
            pltpu.VMEM((2, 3 * FC, MTOK), BF),
            pltpu.VMEM((D, 2 * FC), BF),
            pltpu.VMEM((2, D, MTOK), F32),
            pltpu.VMEM((D, SH), BF), pltpu.VMEM((D, SH), BF), pltpu.VMEM((SH, D), BF),
            pltpu.VMEM((3, D, FF), F32),
            pltpu.VMEM((FF, LW), BF),
            pltpu.VMEM((FC, LW), BF),
            pltpu.VMEM((3, 2, 128, MTOK), BF),
            pltpu.VMEM((NL, 4, 2, SH, 128), BF),
            pltpu.VMEM((NL, 4, SH, 128), BF),
            pltpu.VMEM((2, NL, 2, SH, 128), BF),
            pltpu.VMEM((NL, 2, SH, 128), BF),
            pltpu.VMEM((2, NL, SH, 128), BF),
            pltpu.VMEM((NL, SH, 128), BF),
            dma((14,)), dma((9,)), dma((4,)), dma((5,)), dma((3 * NP,)), dma((3 * NP,)), dma((4, NP)), dma((4, NP)), dma((NP,)), dma((NP,)),
        ],
        compiler_params=pltpu.CompilerParams(
            collective_id=0, has_side_effects=True, vmem_limit_bytes=40 * 1024 * 1024),
        cost_estimate=pl.CostEstimate(flops=9_000_000_000, bytes_accessed=7_000_000, transcendentals=5_000_000),
    )(*args)
    mid = [pltpu.with_memory_space_constraint(t, pltpu.VMEM) for t in mid]
    return pl.pallas_call(
        finish,
        name="mlp_bwd_finish",
        out_shape=[pltpu.HBM((2, D, MTOK), BF), pltpu.HBM((3, D, SH), F32), pltpu.HBM((1, 3, D, FF), F32)],
        in_specs=[vm] * 4,
        out_specs=[hbm] * 3,
        scratch_shapes=[
            pltpu.VMEM((3, D, SH), F32), dma((6,)),
        ],
        compiler_params=pltpu.CompilerParams(vmem_limit_bytes=16 * 1024 * 1024),
        cost_estimate=pl.CostEstimate(flops=2_000_000, bytes_accessed=5_000_000, transcendentals=0),
    )(*mid)


def solution(mesh):
    def local_step(x_dev, dy_dev, gate_shard, up_shard, down_shard, g_dev):
        dx_t, grad_next, grad_layer = fused(
            jnp.swapaxes(x_dev, 1, 2), jnp.swapaxes(dy_dev, 1, 2), gate_shard, up_shard, down_shard, g_dev)
        return jnp.swapaxes(dx_t, 1, 2), grad_next, grad_layer

    in_specs = (P(None, TOK_AXES, None), P(None, TOK_AXES, None), P(None, GROUP_AXES), P(None, GROUP_AXES), P(GROUP_AXES, None), P(TOK_AXES, None, None, None))
    out_specs = (P(None, TOK_AXES, None), P(None, None, GROUP_AXES), P(TOK_AXES, None, None, None))
    return jax.shard_map(local_step, mesh=mesh, in_specs=in_specs, out_specs=out_specs, check_vma=False)
```
